512 devices in a mesh: pair: 16 (over y, x), virt: 32 (over z, core).
Axes of the slice: x: 4, y: 4, z: 16, core: 2. Of those that a mesh axis runs over, the one named last changes fastest.
Arguments:
- density_row_blocks: bfloat16 [640, 512, 2744], P('pair', 'virt'), may hold values from -6 to 6
- vir_left: bfloat16 [512, 2744], P('virt'), may hold values from -0.01171875 to 0.01171875
- vir_right: bfloat16 [512, 2744], P('virt'), may hold values from -0.109375 to 0.109375
- orb_energy: bfloat16 [512], P('virt'), may hold values from 0.5 to 3
- state_energy: float32 [8], replicated, may hold values from -1 to -0.1
- bra_ket_states: int32 [640, 2], P('pair'), may hold values from 0 to 7
- row_block_starts: int32 [640], P('pair'), may hold values from 0 to 2232
Outputs:
- slot_couplings: float32 [640], P('pair')
- heff: float32 [8, 8], replicated
The draws below stay inside these ranges and needn't reach their ends.
All inputs are finite; a program needn't handle non-finite values.
Results may differ from the reference program's by a relative error of at most 0.0003.
Values may be sent and summed in bfloat16 or wider, within the bound.
A program may use at most 64 MiB of HBM per device.

```python
import jax
import jax.numpy as jnp
from jax import lax

MODEL_STATES = 8
ACTIVE_TRIPLES = 2744
NV = 512
BLOCK_ROW_COUNT = 512
DENSITY_BLOCKS = 640


def touch_ends(entries, stream_key, least, largest):
    longest = entries.shape.index(max(entries.shape))
    spots = []
    for shift in (0, 1):
        where = [jax.random.randint(jax.random.fold_in(stream_key, axis), (), 0, length) for axis, length in enumerate(entries.shape)]
        where[longest] = (where[longest] + shift) % entries.shape[longest]
        spots.append(tuple(where))
    return entries.at[spots[0]].set(least).at[spots[1]].set(largest)


def levels(own_key, shape, shards, low, largest):
    factor_of, own = 1.0, jax.random.fold_in(own_key, 6)
    for axis_at, blocks in shards:
        heights = jnp.exp(jax.random.uniform(jax.random.fold_in(own, axis_at), (blocks,), jnp.float32, low / len(shards), largest / len(shards)))
        factor_of = factor_of * jnp.repeat(heights, shape[axis_at] // blocks).reshape([-1 if axis == axis_at else 1 for axis in range(len(shape))])
    return factor_of


def normal_values(own_key, shape, spread, bound, shards=(), kind=jnp.bfloat16):
    drawn = jax.random.normal(own_key, shape, jnp.float32) * spread
    if len(shards) > 0:
        drawn = levels(own_key, shape, shards, -0.22, 0.18) * drawn
    return jnp.clip(drawn, min=-bound, max=bound).astype(kind)


def setup_inputs(seed: int = 0) -> dict:
    arg_keys = jax.random.split(jax.random.key(seed), 8)
    density_row_blocks = normal_values(arg_keys[0], (DENSITY_BLOCKS, BLOCK_ROW_COUNT, ACTIVE_TRIPLES), 1.0, 6.0, ((0, 16), (1, 32)))
    vir_left = normal_values(arg_keys[1], (NV, ACTIVE_TRIPLES), (BLOCK_ROW_COUNT * NV) ** -0.5, 0.01171875, ((0, 32),))
    vir_right = normal_values(arg_keys[2], (NV, ACTIVE_TRIPLES), ACTIVE_TRIPLES ** -0.5, 0.109375, ((0, 32),))
    orb_energy = jnp.clip(0.5 + 2.5 * jax.random.uniform(arg_keys[3], (NV,), jnp.float32) ** levels(arg_keys[3], (NV,), ((0, 32),), -0.2, 0.2), 0.5, 3.0).astype(jnp.bfloat16)
    state_energy = jnp.clip(jax.random.uniform(arg_keys[4], (MODEL_STATES,), jnp.float32, -1.0, -0.1), -1.0, -0.1)
    bra_ket_states = touch_ends(jax.random.randint(arg_keys[5], (DENSITY_BLOCKS, 2), 0, MODEL_STATES), jax.random.fold_in(arg_keys[5], 1), 0, MODEL_STATES - 1).astype(jnp.int32)
    row_block_starts = touch_ends(jax.random.randint(arg_keys[6], (DENSITY_BLOCKS,), 0, ACTIVE_TRIPLES - BLOCK_ROW_COUNT + 1), jax.random.fold_in(arg_keys[6], 1), 0, ACTIVE_TRIPLES - BLOCK_ROW_COUNT).astype(jnp.int32)
    return dict(density_row_blocks=density_row_blocks, vir_left=vir_left, vir_right=vir_right, orb_energy=orb_energy, state_energy=state_energy, bra_ket_states=bra_ket_states, row_block_starts=row_block_starts)


def reference(density_row_blocks, vir_left, vir_right, orb_energy, state_energy, bra_ket_states, row_block_starts):
    block_rows = density_row_blocks.shape[1]
    energy = orb_energy.astype(jnp.float32)

    def single(items):
        block, couple, offset = items
        columns = lax.dynamic_slice_in_dim(vir_left, offset.astype(jnp.int32), block_rows, 1)
        contracted = jnp.dot(vir_right, block.T, preferred_element_type=jnp.float32)
        shift = state_energy[couple[0]] + state_energy[couple[1]]
        inverse = 1.0 / (energy - shift)
        return jnp.sum(columns.astype(jnp.float32) * contracted * inverse[:, None])

    couplings = lax.map(single, (density_row_blocks, bra_ket_states, row_block_starts))
    states = jnp.arange(MODEL_STATES, dtype=jnp.int32)
    first = (bra_ket_states[:, 0:1] == states[None, :]).astype(jnp.float32)
    second = (bra_ket_states[:, 1:2] == states[None, :]).astype(jnp.float32)
    coupling_sum = jnp.dot(first.T, couplings[:, None] * second, precision=lax.Precision.HIGHEST)
    heff = jnp.diag(state_energy) + 0.5 * (coupling_sum + coupling_sum.T)
    return couplings, heff
```

```python
import jax
import jax.numpy as jnp
from jax import lax
from jax.experimental import pallas as pl
from jax.experimental.pallas import tpu as pltpu
from jax.sharding import PartitionSpec as P

MESH = pl.DeviceIdType.MESH
F32, BF16, I32 = jnp.float32, jnp.bfloat16, jnp.int32
SIDE = 4
LONG = 16
LANES = 128
OWN = 12


def nt(a, b):
    return lax.dot_general(a, b, (((1,), (1,)), ((), ())), preferred_element_type=F32)


def kernel(
    starts, states, levels, states_v, energy, left_hbm, right_hbm, dens_hbm,
    coup_ref, heff_ref,
    lv, rv, dens, pick, gp, gz, acc_l, acc_t, part, cbuf, hbuf,
    load_sem, dens_send, dens_recv,
    zs_send, zs_recv, zp_send, zp_recv, p1_send, p1_recv, p2_send, p2_recv,
    c_send, c_recv, h_send, h_recv,
):
    slots, rows, ntrip = dens_hbm.shape
    tiles = -(-ntrip // LANES)
    wide = tiles * LANES
    full = ntrip // LANES * LANES
    rest = ntrip - full
    pair = lax.axis_index("pair")
    virt = lax.axis_index("virt")
    y, x = pair // SIDE, lax.rem(pair, SIDE)
    z, core = virt // 2, lax.rem(virt, 2)

    def at(yy, xx, zz, cc):
        return (yy * SIDE + xx, zz * 2 + cc)

    def turn(v, by, n):
        return lax.rem(v + by + n, n)

    loads = [
        pltpu.make_async_copy(left_hbm, lv, load_sem.at[0]),
        pltpu.make_async_copy(right_hbm, rv, load_sem.at[1]),
        pltpu.make_async_copy(dens_hbm, dens.at[core], load_sem.at[2]),
    ]
    for c in loads:
        c.start()
    barrier = pltpu.get_barrier_semaphore()
    up = at(y, x, turn(z, 1, LONG), core)
    down = at(y, x, turn(z, -1, LONG), core)
    other = at(y, x, z, 1 - core)
    near = [up, down, other]
    near += [at(y, turn(x, j, SIDE), z, core) for j in (1, 2, 3)]
    near += [at(turn(y, j, SIDE), x, z, core) for j in (1, 2, 3)]
    for d in near:
        pl.semaphore_signal(barrier, inc=1, device_id=d, device_id_type=MESH)

    loads[0].wait()
    loads[1].wait()
    eye = lax.broadcasted_iota(I32, (rows, rows), 0) == lax.broadcasted_iota(I32, (rows, rows), 1)
    ecol = jnp.sum(jnp.where(eye, energy[...], 0.0), axis=1, keepdims=True)
    col = lax.broadcasted_iota(I32, (rows, LANES), 1)
    pad = jnp.zeros((rows, LANES - rest), F32)

    def put(t, value):
        if t < 2 * SIDE * SIDE:
            gp[0, t // (2 * SIDE), t // 2 % SIDE, t % 2] = value
        else:
            gz[0, t - 2 * SIDE * SIDE] = value

    for src, base in ((lv, 0), (rv, tiles)):
        for t in range(tiles - 1):
            put(base + t, src[:, t * LANES : (t + 1) * LANES])
        last = jnp.concatenate([src[:, full:ntrip].astype(F32), pad], axis=1)
        if base == 0:
            last = jnp.where(col == rest, ecol, last)
        put(base + tiles - 1, last.astype(BF16))

    pl.semaphore_wait(barrier, len(near))

    def send(src, dst, ssem, rsem, dev):
        return pltpu.make_async_remote_copy(
            src_ref=src, dst_ref=dst, send_sem=ssem, recv_sem=rsem, device_id=dev, device_id_type=MESH
        )

    def slot_of(way, k):
        return k if way == 0 else jnp.where(k == 0, 0, k + 8)

    def stripe(way, k):
        dst = slot_of(way, k + 1)
        return send(
            gp.at[slot_of(way, k), y, x], gp.at[dst, y, x],
            zs_send.at[dst], zs_recv.at[dst], up if way == 0 else down,
        )

    def lane(way, k):
        dst = slot_of(way, k + 1)
        return send(
            gz.at[slot_of(way, k)], gz.at[dst],
            zp_send.at[dst], zp_recv.at[dst], up if way == 0 else down,
        )

    def first(way, k, j):
        s = slot_of(way, k)
        dev = at(y, turn(x, j, SIDE), z, core) if way == 0 else at(turn(y, j, SIDE), x, z, core)
        return send(gp.at[s, y, x], gp.at[s, y, x], p1_send.at[s, j - 1], p1_recv.at[s, j - 1], dev)

    def second(way, k, j):
        s = slot_of(way, k)
        if way == 0:
            ref, dev = gp.at[s, y], at(turn(y, j, SIDE), x, z, core)
        else:
            ref, dev = gp.at[s, :, x], at(y, turn(x, j, SIDE), z, core)
        return send(ref, ref, p2_send.at[s, j - 1], p2_recv.at[s, j - 1], dev)

    def first_in(way, k, j):
        s = slot_of(way, k)
        ref = gp.at[s, y, turn(x, -j, SIDE)] if way == 0 else gp.at[s, turn(y, -j, SIDE), x]
        return send(ref, ref, p1_send.at[s, j - 1], p1_recv.at[s, j - 1], other)

    def second_in(way, k, j):
        s = slot_of(way, k)
        ref = gp.at[s, turn(y, -j, SIDE)] if way == 0 else gp.at[s, :, turn(x, -j, SIDE)]
        return send(ref, ref, p2_send.at[s, j - 1], p2_recv.at[s, j - 1], other)

    for way in (0, 1):
        stripe(way, 0).start()
    for way in (0, 1):
        lane(way, 0).start()
    give = send(dens_hbm, dens.at[core], dens_send.at[0], dens_recv.at[0], other)
    give.start()

    ahead = lax.broadcasted_iota(I32, (rows, wide), 1) - lax.broadcasted_iota(I32, (rows, wide), 0)

    def fill(i, carry):
        at_col = starts[lax.rem(i, slots)] + rows * (2 * z + i // slots)
        pick[i] = jnp.where(ahead == at_col, 1.0, 0.0).astype(BF16)
        return carry

    lax.fori_loop(0, 2 * slots, fill, 0)
    pick[2 * slots] = jnp.where(ahead == ntrip, 1.0, 0.0).astype(BF16)

    def step(k, carry):
        for way in (0, 1):
            stripe(way, k - 1).wait_recv()
            if way == 0:
                stripe(way, k).start()
            else:
                @pl.when(k < 7)
                def _():
                    stripe(1, k).start()
            for j in (2, 1, 3):
                first(way, k, j).start()
        for way in (0, 1):
            lane(way, k - 1).wait_recv()
            if way == 0:
                lane(way, k).start()
            else:
                @pl.when(k < 7)
                def _():
                    lane(1, k).start()

        @pl.when(k > 1)
        def _():
            for way in (0, 1):
                for j in (1, 2, 3):
                    first_in(way, k - 1, j).wait_recv()
                for j in (2, 1, 3):
                    second(way, k - 1, j).start()
        return carry

    lax.fori_loop(1, 8, step, 0)
    stripe(0, 7).wait_recv()
    for j in (2, 1, 3):
        first(0, 8, j).start()
    for way, k in ((0, 7), (1, 7), (0, 8)):
        for j in (1, 2, 3):
            first_in(way, k, j).wait_recv()
        for j in (2, 1, 3):
            second(way, k, j).start()
    lane(0, 7).wait_recv()

    def arrived(k, carry):
        for way in (0, 1):
            for j in (1, 2, 3):
                second_in(way, k, j).wait_recv()
        return carry

    lax.fori_loop(1, 8, arrived, 0)
    for j in (1, 2, 3):
        second_in(0, 8, j).wait_recv()
    loads[2].wait()
    give.wait_recv()

    def two(t):
        halves = []
        for u in (t, t + 1):
            if u < 2 * SIDE * SIDE:
                v = gp[:, u // (2 * SIDE), u // 2 % SIDE, u % 2]
            else:
                v = gz[:, u - 2 * SIDE * SIDE]
            halves.append(v.reshape(LONG * rows, LANES))
        return jnp.concatenate(halves, axis=1)

    for m in range(tiles // 2):
        cols = slice(2 * m * LANES, 2 * (m + 1) * LANES)
        got = nt(pick[:, :, cols].reshape((2 * slots + 1) * rows, 2 * LANES), two(2 * m))
        if m == 0:
            acc_l[...] = got
        else:
            acc_l[...] += got
    for m in range(tiles // 2):
        if m < tiles // 2 - 1:
            d = dens[:, :, :, 2 * m * LANES : 2 * (m + 1) * LANES].reshape(2 * slots * rows, 2 * LANES)
        else:
            d = dens[:, :, :, 2 * m * LANES : ntrip].reshape(2 * slots * rows, ntrip - 2 * m * LANES)
            d = jnp.concatenate([d, jnp.zeros((2 * slots * rows, wide - ntrip), BF16)], axis=1)
        got = nt(d, two(tiles + 2 * m))
        if m == 0:
            acc_t[...] = got
        else:
            acc_t[...] += got

    erow = jnp.broadcast_to(acc_l[2 * slots * rows : 2 * slots * rows + 1, :], (8, LONG * rows))

    def couple(s, carry):
        shift = levels[states[0, s]] + levels[states[1, s]]
        inv = 1.0 / (erow - shift)
        p = pl.multiple_of(s * rows, rows)
        q = pl.multiple_of((s + slots) * rows, rows)
        v = acc_l[pl.ds(p, rows), :] * acc_t[pl.ds(p, rows), :]
        v += acc_l[pl.ds(q, rows), :] * acc_t[pl.ds(q, rows), :]
        w = (v[:8] + v[8:]) * inv
        part[s] = w[:, :LANES] + w[:, LANES:]
        return carry

    lax.fori_loop(0, slots, couple, 0, unroll=4)
    ccol = jnp.sum(jnp.sum(part[...], axis=1), axis=1, keepdims=True)
    diag = lax.broadcasted_iota(I32, (slots, LANES), 0) == lax.broadcasted_iota(I32, (slots, LANES), 1)
    cbuf[virt] = jnp.sum(jnp.where(diag, ccol, 0.0), axis=0, keepdims=True)

    nv = 2 * LONG

    def couplings(j):
        dev = (pair, lax.rem(virt + j, nv))
        return send(cbuf.at[virt], cbuf.at[virt], c_send.at[j], c_recv.at[j], dev)

    def couplings_in(j):
        ref = cbuf.at[lax.rem(virt + nv - j, nv)]
        return send(ref, ref, c_send.at[j], c_recv.at[j], other)

    def go(j, carry):
        couplings(j).start()
        return carry

    def come(j, carry):
        couplings_in(j).wait_recv()
        return carry

    lax.fori_loop(1, nv, go, 0)
    lax.fori_loop(1, nv, come, 0)
    total = jnp.sum(cbuf[...], axis=0)
    coup_ref[...] = total[:, :slots]

    c = total[:, :slots]
    bra, ket = states_v[0:1, :], states_v[1:2, :]
    state = lax.broadcasted_iota(I32, (8, slots), 0)
    side = lax.broadcasted_iota(I32, (8, LANES), 1)
    by_bra = jnp.where(state == bra, c, 0.0)
    by_ket = jnp.where(state == ket, c, 0.0)
    local = jnp.zeros((8, LANES), F32)
    for n in range(8):
        sums = jnp.sum(
            jnp.where(ket == n, by_bra, 0.0) + jnp.where(bra == n, by_ket, 0.0), axis=1, keepdims=True
        )
        local = jnp.where(side == n, sums, local)
    hbuf[pair] = local
    np_ = SIDE * SIDE

    def plane(j):
        dev = (lax.rem(pair + j, np_), virt)
        return send(hbuf.at[pair], hbuf.at[pair], h_send.at[j], h_recv.at[j], dev)

    def plane_in(j):
        ref = hbuf.at[lax.rem(pair + np_ - j, np_)]
        return send(ref, ref, h_send.at[j], h_recv.at[j], other)

    for j in range(1, np_):
        plane(j).start()

    give.wait_send()

    def left(k, carry):
        for way in (0, 1):
            stripe(way, k - 1).wait_send()
            lane(way, k - 1).wait_send()
            for j in (1, 2, 3):
                first(way, k, j).wait_send()
                second(way, k, j).wait_send()
        return carry

    lax.fori_loop(1, 8, left, 0)
    stripe(0, 7).wait_send()
    lane(0, 7).wait_send()
    for j in (1, 2, 3):
        first(0, 8, j).wait_send()
        second(0, 8, j).wait_send()

    def gone(j, carry):
        couplings(j).wait_send()
        return carry

    lax.fori_loop(1, nv, gone, 0)

    for j in range(1, np_):
        plane_in(j).wait_recv()
    square = jnp.sum(hbuf[...], axis=0)[:, :8]
    one = lax.broadcasted_iota(I32, (8, 8), 0)
    two_ = lax.broadcasted_iota(I32, (8, 8), 1)
    out = 0.5 * square
    for n in range(8):
        out += jnp.where((one == n) & (two_ == n), levels[n], 0.0)
    heff_ref[...] = out
    for j in range(1, np_):
        plane(j).wait_send()


def local(density, left, right, energy, levels, states, starts):
    slots, rows, ntrip = density.shape
    n = rows * LONG
    wide = -(-ntrip // LANES) * LANES
    smem, vmem, hbm = (pl.BlockSpec(memory_space=m) for m in (pltpu.SMEM, pltpu.VMEM, pl.ANY))
    dma, reg = pltpu.SemaphoreType.DMA, pltpu.SemaphoreType.REGULAR
    pair_states = states.T
    couplings, heff = pl.pallas_call(
        kernel,
        out_shape=(jax.ShapeDtypeStruct((1, slots), F32), jax.ShapeDtypeStruct((8, 8), F32)),
        in_specs=[smem, smem, smem, vmem, vmem, hbm, hbm, hbm],
        out_specs=(vmem, vmem),
        scratch_shapes=[
            pltpu.VMEM((rows, ntrip), BF16),
            pltpu.VMEM((rows, ntrip), BF16),
            pltpu.VMEM((2, slots, rows, ntrip), BF16),
            pltpu.VMEM((2 * slots + 1, rows, wide), BF16),
            pltpu.VMEM((LONG, SIDE, SIDE, 2, rows, LANES), BF16),
            pltpu.VMEM((LONG, OWN, rows, LANES), BF16),
            pltpu.VMEM(((2 * slots + 1) * rows, n), F32),
            pltpu.VMEM((2 * slots * rows, n), F32),
            pltpu.VMEM((slots, 8, LANES), F32),
            pltpu.VMEM((2 * LONG, 1, LANES), F32),
            pltpu.VMEM((SIDE * SIDE, 8, LANES), F32),
            dma((3,)), dma((1,)), dma((1,)),
            dma((LONG,)), dma((LONG,)), dma((LONG,)), dma((LONG,)),
            dma((LONG, 3)), dma((LONG, 3)), dma((LONG, 3)), dma((LONG, 3)),
            dma((2 * LONG,)), dma((2 * LONG,)), dma((SIDE * SIDE,)), dma((SIDE * SIDE,)),
        ],
        compiler_params=pltpu.CompilerParams(
            collective_id=0, has_side_effects=True, vmem_limit_bytes=52 * 1024 * 1024
        ),
    )(
        starts, pair_states, levels, pair_states, energy.astype(F32).reshape(1, rows),
        left, right, density,
    )
    return couplings.reshape(slots), heff


def solution(mesh):
    placed = (
        P("pair", "virt", None),
        P("virt", None),
        P("virt", None),
        P("virt"),
        P(),
        P("pair", None),
        P("pair"),
    )
    return jax.shard_map(
        local, mesh=mesh, in_specs=placed, out_specs=(P("pair"), P()), check_vma=False
    )
```

```python
import jax
import jax.numpy as jnp
from jax import lax
from jax.experimental import pallas as pl
from jax.experimental.pallas import tpu as pltpu
from jax.sharding import PartitionSpec as P

MESH = pl.DeviceIdType.MESH
F32, BF16, I32 = jnp.float32, jnp.bfloat16, jnp.int32
SIDE = 4
LONG = 16
LANES = 128
OWN = 12
CUTS = 3
GIVES = 8


def nt(a, b):
    return lax.dot_general(a, b, (((1,), (1,)), ((), ())), preferred_element_type=F32)


def kernel(
    starts_hbm, states_hbm, levels_hbm, energy_hbm, left_hbm, right_hbm, dens_hbm,
    coup_ref, heff_ref,
    starts, states, levels, states_v, energy, lv, rv, dens, pick, gp, gz, acc_l, acc_t, part, cbuf, hbuf,
    load_sem, dens_send, dens_recv,
    zs_send, zs_recv, zp_send, zp_recv, p1_send, p1_recv, p2_send, p2_recv,
    c_send, c_recv, h_send, h_recv,
):
    slots, rows, ntrip = dens_hbm.shape
    tiles = -(-ntrip // LANES)
    wide = tiles * LANES
    full = ntrip // LANES * LANES
    rest = ntrip - full
    pair = lax.axis_index("pair")
    virt = lax.axis_index("virt")
    y, x = pair // SIDE, lax.rem(pair, SIDE)
    z, core = virt // 2, lax.rem(virt, 2)

    def at(yy, xx, zz, cc):
        return (yy * SIDE + xx, zz * 2 + cc)

    def turn(v, by, n):
        return lax.rem(v + by + n, n)

    barrier = pltpu.get_barrier_semaphore()
    up = at(y, x, turn(z, 1, LONG), core)
    down = at(y, x, turn(z, -1, LONG), core)
    other = at(y, x, z, 1 - core)
    up2 = at(y, x, turn(z, 2, LONG), core)
    down2 = at(y, x, turn(z, -2, LONG), core)
    near = [up, down, up2, down2, other]
    near += [at(y, turn(x, j, SIDE), z, core) for j in (1, 2, 3)]
    near += [at(turn(y, j, SIDE), x, z, core) for j in (1, 2, 3)]
    for d in near:
        pl.semaphore_signal(barrier, inc=1, device_id=d, device_id_type=MESH)

    loads = [
        pltpu.make_async_copy(src, dst, load_sem.at[n])
        for n, (src, dst) in enumerate((
            (left_hbm, lv), (right_hbm, rv), (dens_hbm, dens.at[core]), (energy_hbm, energy),
            (starts_hbm, starts), (states_hbm, states), (levels_hbm, levels), (states_hbm, states_v),
        ))
    ]
    for n in (0, 1, 3, 4, 5, 6, 7, 2):
        loads[n].start()

    for n in (0, 1, 3):
        loads[n].wait()
    eye = lax.broadcasted_iota(I32, (rows, rows), 0) == lax.broadcasted_iota(I32, (rows, rows), 1)
    ecol = jnp.sum(jnp.where(eye, energy[...].astype(F32).reshape(1, rows), 0.0), axis=1, keepdims=True)
    col = lax.broadcasted_iota(I32, (rows, LANES), 1)
    pad = jnp.zeros((rows, LANES - rest), F32)

    def put(t, value):
        if t < 2 * SIDE * SIDE:
            gp[0, t // (2 * SIDE), t // 2 % SIDE, t % 2] = value
        else:
            gz[0, t - 2 * SIDE * SIDE] = value

    for src, base in ((lv, 0), (rv, tiles)):
        for t in range(tiles - 1):
            put(base + t, src[:, t * LANES : (t + 1) * LANES])
        last = jnp.concatenate([src[:, full:ntrip].astype(F32), pad], axis=1)
        if base == 0:
            last = jnp.where(col == rest, ecol, last)
        put(base + tiles - 1, last.astype(BF16))

    pl.semaphore_wait(barrier, len(near))

    def send(src, dst, ssem, rsem, dev):
        return pltpu.make_async_remote_copy(
            src_ref=src, dst_ref=dst, send_sem=ssem, recv_sem=rsem, device_id=dev, device_id_type=MESH
        )

    ends = (8, 7)

    def slot_of(way, k):
        return k if way == 0 or k == 0 else k + 8

    def stripe(way, k, hops):
        dst = slot_of(way, k + hops)
        dev = ((up, up2), (down, down2))[way][hops - 1]
        return send(
            gp.at[slot_of(way, k), y, x], gp.at[dst, y, x], zs_send.at[dst], zs_recv.at[dst], dev
        )

    def stripe_to(way, k):
        hops = 2 - k % 2
        return stripe(way, k - hops, hops)

    def forward(way, k):
        for hops in (2, 1):
            if k + hops <= ends[way]:
                stripe(way, k, hops).start()

    def lane(way, k, hops, cut):
        dst = slot_of(way, k + hops)
        dev = ((up, up2), (down, down2))[way][hops - 1]
        part_of = pl.ds(cut * (OWN // CUTS), OWN // CUTS)
        return send(
            gz.at[slot_of(way, k), part_of], gz.at[dst, part_of],
            zp_send.at[dst, cut], zp_recv.at[dst, cut], dev,
        )

    def lane_to(way, k, cut):
        hops = 2 - k % 2
        return lane(way, k - hops, hops, cut)

    def lanes(k):
        for cut in range(CUTS):
            for way in (0, 1):
                if 0 < k <= ends[way]:
                    lane_to(way, k, cut).wait_recv()
                if k + 2 <= ends[way]:
                    lane(way, k, 2, cut).start()
        for cut in range(CUTS):
            for way in (0, 1):
                if k + 1 <= ends[way]:
                    lane(way, k, 1, cut).start()

    def give(g):
        part_of = pl.ds(g * (slots // GIVES), slots // GIVES)
        return send(
            dens_hbm.at[part_of], dens.at[core, part_of], dens_send.at[g], dens_recv.at[g], other
        )

    def first(way, k, j):
        s = slot_of(way, k)
        dev = at(y, turn(x, j, SIDE), z, core) if way == 0 else at(turn(y, j, SIDE), x, z, core)
        return send(gp.at[s, y, x], gp.at[s, y, x], p1_send.at[s, j - 1], p1_recv.at[s, j - 1], dev)

    def second(way, k, j):
        s = slot_of(way, k)
        if way == 0:
            ref, dev = gp.at[s, y], at(turn(y, j, SIDE), x, z, core)
        else:
            ref, dev = gp.at[s, :, x], at(y, turn(x, j, SIDE), z, core)
        return send(ref, ref, p2_send.at[s, j - 1], p2_recv.at[s, j - 1], dev)

    def first_in(way, k, j):
        s = slot_of(way, k)
        ref = gp.at[s, y, turn(x, -j, SIDE)] if way == 0 else gp.at[s, turn(y, -j, SIDE), x]
        return send(ref, ref, p1_send.at[s, j - 1], p1_recv.at[s, j - 1], other)

    def second_in(way, k, j):
        s = slot_of(way, k)
        ref = gp.at[s, turn(y, -j, SIDE)] if way == 0 else gp.at[s, :, turn(x, -j, SIDE)]
        return send(ref, ref, p2_send.at[s, j - 1], p2_recv.at[s, j - 1], other)

    for way in (0, 1):
        forward(way, 0)
    lanes(0)

    for n in (4, 5, 6, 7):
        loads[n].wait()

    ahead = lax.broadcasted_iota(I32, (rows, wide), 1) - lax.broadcasted_iota(I32, (rows, wide), 0)

    def fill(i, carry):
        at_col = starts[lax.rem(i, slots)] + rows * (2 * z + i // slots)
        pick[i] = jnp.where(ahead == at_col, 1.0, 0.0).astype(BF16)
        return carry

    lax.fori_loop(0, 2 * slots, fill, 0)
    pick[2 * slots] = jnp.where(ahead == ntrip, 1.0, 0.0).astype(BF16)

    def plane_on(s):
        for k in (2 * s - 1, 2 * s):
            for way in (0, 1):
                if k <= ends[way]:
                    for j in (1, 2, 3):
                        first_in(way, k, j).wait_recv()
                    for j in (2, 1, 3):
                        second(way, k, j).start()

    for s in (1, 2, 3, 4):
        for k in (2 * s - 1, 2 * s):
            for way in (0, 1):
                if k <= ends[way]:
                    stripe_to(way, k).wait_recv()
                    if k % 2 == 0:
                        forward(way, k)
                    for j in (2, 1, 3):
                        first(way, k, j).start()
        lanes(2 * s)
        if s > 1:
            plane_on(s - 1)
        for g in range((s - 1) * GIVES // 4, s * GIVES // 4):
            give(g).start()
    plane_on(4)
    for k in (1, 3, 5, 7):
        for way in (0, 1):
            for cut in range(CUTS):
                lane_to(way, k, cut).wait_recv()
    loads[2].wait()
    for g in range(GIVES):
        give(g).wait_recv()

    alone = (2 * SIDE * SIDE - tiles) // 2

    def two(t):
        halves = []
        for u in (t, t + 1):
            if u < 2 * SIDE * SIDE:
                v = gp[:, u // (2 * SIDE), u // 2 % SIDE, u % 2]
            else:
                v = gz[:, u - 2 * SIDE * SIDE]
            halves.append(v.reshape(LONG * rows, LANES))
        return jnp.concatenate(halves, axis=1)

    half = slots * rows

    def add(acc, lo, got, fresh):
        if fresh:
            acc[lo : lo + got.shape[0], :] = got
        else:
            acc[lo : lo + got.shape[0], :] += got

    def contract(m, fresh):
        b = two(tiles + 2 * m)
        for h in (0, 1):
            if m < tiles // 2 - 1:
                d = dens[h, :, :, 2 * m * LANES : 2 * (m + 1) * LANES].reshape(half, 2 * LANES)
            else:
                d = dens[h, :, :, 2 * m * LANES : ntrip].reshape(half, ntrip - 2 * m * LANES)
                d = jnp.concatenate([d, jnp.zeros((half, wide - ntrip), BF16)], axis=1)
            add(acc_t, h * half, nt(d, b), fresh)

    def select(m, fresh):
        cols = slice(2 * m * LANES, 2 * (m + 1) * LANES)
        b = two(2 * m)
        for h in (0, 1):
            lo, hi = h * slots, (h + 1) * slots + h
            d = pick[lo:hi, :, cols].reshape((hi - lo) * rows, 2 * LANES)
            add(acc_l, lo * rows, nt(d, b), fresh)

    for m in range(alone, tiles // 2):
        contract(m, m == alone)
    for k in range(1, 9):
        for way in (0, 1):
            if k <= ends[way]:
                for j in (1, 2, 3):
                    second_in(way, k, j).wait_recv()
    for m in range(tiles // 2):
        select(m, m == 0)
    for m in range(alone):
        contract(m, False)

    erow = jnp.broadcast_to(acc_l[2 * slots * rows : 2 * slots * rows + 1, :], (8, LONG * rows))

    def couple(s, carry):
        shift = levels[states[0, s]] + levels[states[1, s]]
        inv = 1.0 / (erow - shift)
        p = pl.multiple_of(s * rows, rows)
        q = pl.multiple_of((s + slots) * rows, rows)
        v = acc_l[pl.ds(p, rows), :] * acc_t[pl.ds(p, rows), :]
        v += acc_l[pl.ds(q, rows), :] * acc_t[pl.ds(q, rows), :]
        w = (v[:8] + v[8:]) * inv
        part[s] = w[:, :LANES] + w[:, LANES:]
        return carry

    lax.fori_loop(0, slots, couple, 0, unroll=4)
    ccol = jnp.sum(jnp.sum(part[...], axis=1), axis=1, keepdims=True)
    diag = lax.broadcasted_iota(I32, (slots, LANES), 0) == lax.broadcasted_iota(I32, (slots, LANES), 1)
    cbuf[virt] = jnp.sum(jnp.where(diag, ccol, 0.0), axis=0, keepdims=True)

    nv = 2 * LONG

    def couplings(j):
        dev = (pair, lax.rem(virt + j, nv))
        return send(cbuf.at[virt], cbuf.at[virt], c_send.at[j], c_recv.at[j], dev)

    def couplings_in(j):
        ref = cbuf.at[lax.rem(virt + nv - j, nv)]
        return send(ref, ref, c_send.at[j], c_recv.at[j], other)

    def go(j, carry):
        couplings(j).start()
        return carry

    def come(j, carry):
        couplings_in(j).wait_recv()
        return carry

    lax.fori_loop(1, nv, go, 0)
    lax.fori_loop(1, nv, come, 0)
    total = jnp.sum(cbuf[...], axis=0)
    coup_ref[...] = total[:, :slots]

    c = total[:, :slots]
    bra, ket = states_v[0:1, :], states_v[1:2, :]
    state = lax.broadcasted_iota(I32, (8, slots), 0)
    side = lax.broadcasted_iota(I32, (8, LANES), 1)
    by_bra = jnp.where(state == bra, c, 0.0)
    by_ket = jnp.where(state == ket, c, 0.0)
    local = jnp.zeros((8, LANES), F32)
    for n in range(8):
        sums = jnp.sum(
            jnp.where(ket == n, by_bra, 0.0) + jnp.where(bra == n, by_ket, 0.0), axis=1, keepdims=True
        )
        local = jnp.where(side == n, sums, local)
    hbuf[pair] = local
    np_ = SIDE * SIDE

    def plane(j):
        dev = (lax.rem(pair + j, np_), virt)
        return send(hbuf.at[pair], hbuf.at[pair], h_send.at[j], h_recv.at[j], dev)

    def plane_in(j):
        ref = hbuf.at[lax.rem(pair + np_ - j, np_)]
        return send(ref, ref, h_send.at[j], h_recv.at[j], other)

    for j in range(1, np_):
        plane(j).start()

    for g in range(GIVES):
        give(g).wait_send()
    for k in range(1, 9):
        for way in (0, 1):
            if k <= ends[way]:
                stripe_to(way, k).wait_send()
                for cut in range(CUTS):
                    lane_to(way, k, cut).wait_send()
                for j in (1, 2, 3):
                    first(way, k, j).wait_send()
                    second(way, k, j).wait_send()

    def gone(j, carry):
        couplings(j).wait_send()
        return carry

    lax.fori_loop(1, nv, gone, 0)

    for j in range(1, np_):
        plane_in(j).wait_recv()
    square = jnp.sum(hbuf[...], axis=0)[:, :8]
    one = lax.broadcasted_iota(I32, (8, 8), 0)
    two_ = lax.broadcasted_iota(I32, (8, 8), 1)
    out = 0.5 * square
    for n in range(8):
        out += jnp.where((one == n) & (two_ == n), levels[n], 0.0)
    heff_ref[...] = out
    for j in range(1, np_):
        plane(j).wait_send()


def local(density, left, right, energy, levels, states, starts):
    slots, rows, ntrip = density.shape
    n = rows * LONG
    wide = -(-ntrip // LANES) * LANES
    vmem, hbm = (pl.BlockSpec(memory_space=m) for m in (pltpu.VMEM, pl.ANY))
    dma = pltpu.SemaphoreType.DMA
    couplings, heff = pl.pallas_call(
        kernel,
        out_shape=(jax.ShapeDtypeStruct((1, slots), F32), jax.ShapeDtypeStruct((8, 8), F32)),
        in_specs=[hbm] * 7,
        out_specs=(vmem, vmem),
        scratch_shapes=[
            pltpu.SMEM((slots,), I32),
            pltpu.SMEM((2, slots), I32),
            pltpu.SMEM((8,), F32),
            pltpu.VMEM((2, slots), I32),
            pltpu.VMEM((rows,), BF16),
            pltpu.VMEM((rows, ntrip), BF16),
            pltpu.VMEM((rows, ntrip), BF16),
            pltpu.VMEM((2, slots, rows, ntrip), BF16),
            pltpu.VMEM((2 * slots + 1, rows, wide), BF16),
            pltpu.VMEM((LONG, SIDE, SIDE, 2, rows, LANES), BF16),
            pltpu.VMEM((LONG, OWN, rows, LANES), BF16),
            pltpu.VMEM(((2 * slots + 1) * rows, n), F32),
            pltpu.VMEM((2 * slots * rows, n), F32),
            pltpu.VMEM((slots, 8, LANES), F32),
            pltpu.VMEM((2 * LONG, 1, LANES), F32),
            pltpu.VMEM((SIDE * SIDE, 8, LANES), F32),
            dma((8,)), dma((GIVES,)), dma((GIVES,)),
            dma((LONG,)), dma((LONG,)), dma((LONG, CUTS)), dma((LONG, CUTS)),
            dma((LONG, 3)), dma((LONG, 3)), dma((LONG, 3)), dma((LONG, 3)),
            dma((2 * LONG,)), dma((2 * LONG,)), dma((SIDE * SIDE,)), dma((SIDE * SIDE,)),
        ],
        compiler_params=pltpu.CompilerParams(
            collective_id=0, has_side_effects=True, vmem_limit_bytes=67043328
        ),
    )(
        starts, states.T, levels, energy, left, right, density,
    )
    return couplings.reshape(slots), heff


def solution(mesh):
    placed = (
        P("pair", "virt", None),
        P("virt", None),
        P("virt", None),
        P("virt"),
        P(),
        P("pair", None),
        P("pair"),
    )
    return jax.shard_map(
        local, mesh=mesh, in_specs=placed, out_specs=(P("pair"), P()), check_vma=False
    )
```

```python
import jax
import jax.numpy as jnp
from jax import lax
from jax.experimental import pallas as pl
from jax.experimental.pallas import tpu as pltpu
from jax.sharding import PartitionSpec as P

MESH = pl.DeviceIdType.MESH
F32, BF16, I32 = jnp.float32, jnp.bfloat16, jnp.int32
SIDE = 4
LONG = 16
LANES = 128
OWN = 12
CUTS = 3
GIVES = 8


def nt(a, b):
    return lax.dot_general(a, b, (((1,), (1,)), ((), ())), preferred_element_type=F32)


def kernel(
    starts_hbm, states_hbm, levels_hbm, energy_hbm, left_hbm, right_hbm, dens_hbm,
    coup_ref, heff_ref,
    starts, states, levels, states_v, energy, lv, rv, dens, pick, gp, gz, acc_l, acc_t, part, cbuf, hbuf,
    load_sem, send_sem, dens_recv, zs_recv, zp_recv, odd_recv, p1_recv, p2_recv, c_recv, h_recv,
):
    slots, rows, ntrip = dens_hbm.shape
    tiles = -(-ntrip // LANES)
    wide = tiles * LANES
    full = ntrip // LANES * LANES
    rest = ntrip - full
    pair = lax.axis_index("pair")
    virt = lax.axis_index("virt")
    y, x = pair // SIDE, lax.rem(pair, SIDE)
    z, core = virt // 2, lax.rem(virt, 2)

    def at(yy, xx, zz, cc):
        return (yy * SIDE + xx, zz * 2 + cc)

    def turn(v, by, n):
        return lax.rem(v + by + n, n)

    barrier = pltpu.get_barrier_semaphore()
    up = at(y, x, turn(z, 1, LONG), core)
    down = at(y, x, turn(z, -1, LONG), core)
    other = at(y, x, z, 1 - core)
    up2 = at(y, x, turn(z, 2, LONG), core)
    down2 = at(y, x, turn(z, -2, LONG), core)
    near = [up, down, up2, down2, other]
    near += [at(y, turn(x, j, SIDE), z, core) for j in (1, 2, 3)]
    near += [at(turn(y, j, SIDE), x, z, core) for j in (1, 2, 3)]
    for d in near:
        pl.semaphore_signal(barrier, inc=1, device_id=d, device_id_type=MESH)

    loads = [
        pltpu.make_async_copy(src, dst, load_sem.at[n])
        for n, (src, dst) in enumerate((
            (left_hbm, lv), (right_hbm, rv), (dens_hbm, dens.at[core]), (energy_hbm, energy),
            (starts_hbm, starts), (states_hbm, states), (levels_hbm, levels), (states_hbm, states_v),
        ))
    ]
    for n in (0, 1, 3, 4, 5, 6, 7, 2):
        loads[n].start()

    for n in (0, 1, 3):
        loads[n].wait()
    eye = lax.broadcasted_iota(I32, (rows, rows), 0) == lax.broadcasted_iota(I32, (rows, rows), 1)
    ecol = jnp.sum(jnp.where(eye, energy[...].astype(F32).reshape(1, rows), 0.0), axis=1, keepdims=True)
    col = lax.broadcasted_iota(I32, (rows, LANES), 1)
    pad = jnp.zeros((rows, LANES - rest), F32)

    def put(t, value):
        if t < 2 * SIDE * SIDE:
            gp[0, t // (2 * SIDE), t // 2 % SIDE, t % 2] = value
        else:
            gz[0, t - 2 * SIDE * SIDE] = value

    for src, base in ((lv, 0), (rv, tiles)):
        for t in range(tiles - 1):
            put(base + t, src[:, t * LANES : (t + 1) * LANES])
        last = jnp.concatenate([src[:, full:ntrip].astype(F32), pad], axis=1)
        if base == 0:
            last = jnp.where(col == rest, ecol, last)
        put(base + tiles - 1, last.astype(BF16))

    pl.semaphore_wait(barrier, len(near))

    def send(src, dst, ssem, rsem, dev):
        return pltpu.make_async_remote_copy(
            src_ref=src, dst_ref=dst, send_sem=ssem, recv_sem=rsem, device_id=dev, device_id_type=MESH
        )

    def bytes_of(ref, sem):
        pltpu.make_async_copy(ref, ref, sem).wait()

    STRIPE, LANE, FIRST, SECOND, DENS, COUPLE, HEFF = (send_sem.at[n] for n in range(7))
    ends = (8, 7)

    def slot_of(way, k):
        return k if way == 0 or k == 0 else k + 8

    def stripe(way, k, hops):
        dst = slot_of(way, k + hops)
        dev = ((up, up2), (down, down2))[way][hops - 1]
        return send(
            gp.at[slot_of(way, k), y, x], gp.at[dst, y, x], STRIPE, zs_recv.at[dst], dev
        )

    def stripe_to(way, k):
        hops = 2 - k % 2
        return stripe(way, k - hops, hops)

    def forward(way, k):
        for hops in (2, 1):
            if k + hops <= ends[way]:
                stripe(way, k, hops).start()

    def lane(way, k, hops, cut):
        dst = slot_of(way, k + hops)
        dev = ((up, up2), (down, down2))[way][hops - 1]
        part_of = pl.ds(cut * (OWN // CUTS), OWN // CUTS)
        sem = zp_recv.at[(k + hops) // 2 - 1, way, cut] if hops == 2 else odd_recv.at[0]
        return send(gz.at[slot_of(way, k), part_of], gz.at[dst, part_of], LANE, sem, dev)

    def lanes(k):
        for cut in range(CUTS):
            for way in (0, 1):
                if 0 < k <= ends[way]:
                    lane(way, k - 2, 2, cut).wait_recv()
                if k + 2 <= ends[way]:
                    lane(way, k, 2, cut).start()
        for cut in range(CUTS):
            for way in (0, 1):
                if k + 1 <= ends[way]:
                    lane(way, k, 1, cut).start()

    def give(g):
        part_of = pl.ds(g * (slots // GIVES), slots // GIVES)
        return send(
            dens_hbm.at[part_of], dens.at[core, part_of], DENS, dens_recv.at[0], other
        )

    def first(way, k, j):
        s = slot_of(way, k)
        dev = at(y, turn(x, j, SIDE), z, core) if way == 0 else at(turn(y, j, SIDE), x, z, core)
        return send(gp.at[s, y, x], gp.at[s, y, x], FIRST, p1_recv.at[s], dev)

    def second(way, k, j):
        s = slot_of(way, k)
        if way == 0:
            ref, dev = gp.at[s, y], at(turn(y, j, SIDE), x, z, core)
        else:
            ref, dev = gp.at[s, :, x], at(y, turn(x, j, SIDE), z, core)
        return send(ref, ref, SECOND, p2_recv.at[0], dev)

    def first_in(way, k):
        bytes_of(gp.at[slot_of(way, k), 0, 0:3], p1_recv.at[slot_of(way, k)])

    def give_some(n):
        for g in range(n * GIVES // 4, (n + 1) * GIVES // 4):
            give(g).start()

    for way in (0, 1):
        forward(way, 0)
    lanes(0)
    give_some(0)

    for n in (4, 5, 6, 7):
        loads[n].wait()

    ahead = lax.broadcasted_iota(I32, (rows, wide), 1) - lax.broadcasted_iota(I32, (rows, wide), 0)

    def fill(i, carry):
        at_col = starts[lax.rem(i, slots)] + rows * (2 * z + i // slots)
        pick[i] = jnp.where(ahead == at_col, 1.0, 0.0).astype(BF16)
        return carry

    lax.fori_loop(0, 2 * slots, fill, 0)
    pick[2 * slots] = jnp.where(ahead == ntrip, 1.0, 0.0).astype(BF16)

    def plane_on(s):
        for k in (2 * s, 2 * s - 1):
            for way in (0, 1):
                if k <= ends[way]:
                    first_in(way, k)
                    for j in (2, 1, 3):
                        second(way, k, j).start()

    for s in (1, 2, 3, 4):
        for k in (2 * s, 2 * s - 1):
            for way in (0, 1):
                if k <= ends[way]:
                    stripe_to(way, k).wait_recv()
                    if k % 2 == 0:
                        forward(way, k)
                    for j in (2, 1, 3):
                        first(way, k, j).start()
        if s > 1:
            plane_on(s - 1)
        if s < 4:
            lanes(2 * s)
            give_some(s)
    plane_on(4)
    lanes(8)
    bytes_of(gz.at[0:8], odd_recv.at[0])
    loads[2].wait()
    bytes_of(dens.at[0], dens_recv.at[0])

    alone = (2 * SIDE * SIDE - tiles) // 2

    def two(t):
        halves = []
        for u in (t, t + 1):
            if u < 2 * SIDE * SIDE:
                v = gp[:, u // (2 * SIDE), u // 2 % SIDE, u % 2]
            else:
                v = gz[:, u - 2 * SIDE * SIDE]
            halves.append(v.reshape(LONG * rows, LANES))
        return jnp.concatenate(halves, axis=1)

    half = slots * rows

    def add(acc, lo, got, fresh):
        if fresh:
            acc[lo : lo + got.shape[0], :] = got
        else:
            acc[lo : lo + got.shape[0], :] += got

    def contract(m, fresh):
        b = two(tiles + 2 * m)
        for h in (0, 1):
            if m < tiles // 2 - 1:
                d = dens[h, :, :, 2 * m * LANES : 2 * (m + 1) * LANES].reshape(half, 2 * LANES)
            else:
                d = dens[h, :, :, 2 * m * LANES : ntrip].reshape(half, ntrip - 2 * m * LANES)
                d = jnp.concatenate([d, jnp.zeros((half, wide - ntrip), BF16)], axis=1)
            add(acc_t, h * half, nt(d, b), fresh)

    def select(m, fresh):
        cols = slice(2 * m * LANES, 2 * (m + 1) * LANES)
        b = two(2 * m)
        for h in (0, 1):
            lo, hi = h * slots, (h + 1) * slots + h
            d = pick[lo:hi, :, cols].reshape((hi - lo) * rows, 2 * LANES)
            add(acc_l, lo * rows, nt(d, b), fresh)

    for m in range(alone, tiles // 2):
        contract(m, m == alone)
    bytes_of(gp.at[1:LONG, :, 0:3], p2_recv.at[0])
    for m in range(tiles // 2):
        select(m, m == 0)
    for m in range(alone):
        contract(m, False)

    erow = jnp.broadcast_to(acc_l[2 * slots * rows : 2 * slots * rows + 1, :], (8, LONG * rows))

    def couple(s, carry):
        shift = levels[states[0, s]] + levels[states[1, s]]
        inv = 1.0 / (erow - shift)
        p = pl.multiple_of(s * rows, rows)
        q = pl.multiple_of((s + slots) * rows, rows)
        v = acc_l[pl.ds(p, rows), :] * acc_t[pl.ds(p, rows), :]
        v += acc_l[pl.ds(q, rows), :] * acc_t[pl.ds(q, rows), :]
        w = (v[:8] + v[8:]) * inv
        part[s] = w[:, :LANES] + w[:, LANES:]
        return carry

    lax.fori_loop(0, slots, couple, 0, unroll=4)
    ccol = jnp.sum(jnp.sum(part[...], axis=1), axis=1, keepdims=True)
    diag = lax.broadcasted_iota(I32, (slots, LANES), 0) == lax.broadcasted_iota(I32, (slots, LANES), 1)
    cbuf[virt] = jnp.sum(jnp.where(diag, ccol, 0.0), axis=0, keepdims=True)

    nv = 2 * LONG

    def go(j, carry):
        dev = (pair, lax.rem(virt + j, nv))
        send(cbuf.at[virt], cbuf.at[virt], COUPLE, c_recv.at[0], dev).start()
        return carry

    lax.fori_loop(1, nv, go, 0, unroll=True)
    bytes_of(cbuf.at[1:nv], c_recv.at[0])
    total = jnp.sum(cbuf[...], axis=0)
    coup_ref[...] = total[:, :slots]

    c = total[:, :slots]
    bra, ket = states_v[0:1, :], states_v[1:2, :]
    state = lax.broadcasted_iota(I32, (8, slots), 0)
    side = lax.broadcasted_iota(I32, (8, LANES), 1)
    by_bra = jnp.where(state == bra, c, 0.0)
    by_ket = jnp.where(state == ket, c, 0.0)
    local = jnp.zeros((8, LANES), F32)
    for n in range(8):
        sums = jnp.sum(
            jnp.where(ket == n, by_bra, 0.0) + jnp.where(bra == n, by_ket, 0.0), axis=1, keepdims=True
        )
        local = jnp.where(side == n, sums, local)
    hbuf[pair] = local
    np_ = SIDE * SIDE

    for j in range(1, np_):
        dev = (lax.rem(pair + j, np_), virt)
        send(hbuf.at[pair], hbuf.at[pair], HEFF, h_recv.at[0], dev).start()

    bytes_of(gp.at[1:LONG, 0, 0], STRIPE)
    bytes_of(gz.at[1:LONG], LANE)
    bytes_of(gp.at[1:LONG, 0, 0:3], FIRST)
    bytes_of(gp.at[1:LONG, :, 0:3], SECOND)
    bytes_of(dens.at[0], DENS)
    bytes_of(cbuf.at[1:nv], COUPLE)

    bytes_of(hbuf.at[1:np_], h_recv.at[0])
    square = jnp.sum(hbuf[...], axis=0)[:, :8]
    one = lax.broadcasted_iota(I32, (8, 8), 0)
    two_ = lax.broadcasted_iota(I32, (8, 8), 1)
    out = 0.5 * square
    for n in range(8):
        out += jnp.where((one == n) & (two_ == n), levels[n], 0.0)
    heff_ref[...] = out
    bytes_of(hbuf.at[1:np_], HEFF)


def local(density, left, right, energy, levels, states, starts):
    slots, rows, ntrip = density.shape
    n = rows * LONG
    wide = -(-ntrip // LANES) * LANES
    vmem, hbm = (pl.BlockSpec(memory_space=m) for m in (pltpu.VMEM, pltpu.HBM))
    dma = pltpu.SemaphoreType.DMA
    couplings, heff = pl.pallas_call(
        kernel,
        out_shape=(jax.ShapeDtypeStruct((1, slots), F32), jax.ShapeDtypeStruct((8, 8), F32)),
        in_specs=[hbm] * 7,
        out_specs=(vmem, vmem),
        scratch_shapes=[
            pltpu.SMEM((slots,), I32),
            pltpu.SMEM((2, slots), I32),
            pltpu.SMEM((8,), F32),
            pltpu.VMEM((2, slots), I32),
            pltpu.VMEM((rows,), BF16),
            pltpu.VMEM((rows, ntrip), BF16),
            pltpu.VMEM((rows, ntrip), BF16),
            pltpu.VMEM((2, slots, rows, ntrip), BF16),
            pltpu.VMEM((2 * slots + 1, rows, wide), BF16),
            pltpu.VMEM((LONG, SIDE, SIDE, 2, rows, LANES), BF16),
            pltpu.VMEM((LONG, OWN, rows, LANES), BF16),
            pltpu.VMEM(((2 * slots + 1) * rows, n), F32),
            pltpu.VMEM((2 * slots * rows, n), F32),
            pltpu.VMEM((slots, 8, LANES), F32),
            pltpu.VMEM((2 * LONG, 1, LANES), F32),
            pltpu.VMEM((SIDE * SIDE, 8, LANES), F32),
            dma((8,)), dma((7,)), dma((1,)), dma((LONG,)), dma((4, 2, CUTS)), dma((1,)),
            dma((LONG,)), dma((1,)), dma((1,)), dma((1,)),
        ],
        compiler_params=pltpu.CompilerParams(
            collective_id=0, has_side_effects=True, vmem_limit_bytes=67043328
        ),
    )(
        starts, states.T, levels, energy, left, right, density,
    )
    return couplings.reshape(slots), heff


def solution(mesh):
    placed = (
        P("pair", "virt", None),
        P("virt", None),
        P("virt", None),
        P("virt"),
        P(),
        P("pair", None),
        P("pair"),
    )
    return jax.shard_map(
        local, mesh=mesh, in_specs=placed, out_specs=(P("pair"), P()), check_vma=False
    )
```
